32 devices in a mesh: lat: 16 (over z, y, x), batch: 2 (over core).
Axes of the slice: x: 2, y: 2, z: 4, core: 2. Of those that a mesh axis runs over, the one named last changes fastest.
Arguments:
- fields: bfloat16 [2, 192, 384, 384], P('batch', 'lat'), may hold values from -6 to 6
- cotangent: bfloat16 [2, 192, 384, 384], P('batch', 'lat'), may hold values from -6 to 6
- weights: bfloat16 [128, 2, 384, 384], P('lat'), may hold values from -0.21875 to 0.21875
- degree_of: int32 [128], replicated, may hold values from 0 to 127, each once
Outputs:
- grad_fields: bfloat16 [2, 192, 384, 384], P('batch', 'lat')
- grad_weights: bfloat16 [128, 2, 384, 384], P('lat')
The draws below stay inside these ranges and needn't reach their ends.
Inputs may be any that keep to these rules, and one draw needn't show every extreme that they name: `degree_of`: each degree 0 to 127 is held by exactly one slot.
All inputs are finite; a program needn't handle non-finite values.
Results may differ from the reference program's by a relative error of at most 0.018.
Values may be sent and summed in bfloat16 or wider, within the bound.
A program may use at most 64 MiB of HBM per device.

```python
import jax
import jax.numpy as jnp
from jax import lax

LATS = 192
LONS = 384
ORDERS = 128
DEGREES = 128
CHANNELS = 384
BATCH = 2


def shard_levels(key, extent, split, least, largest):
    loudness = 1.0
    for axis_at, blocks in split:
        draws = jax.random.uniform(jax.random.fold_in(jax.random.fold_in(key, 6), axis_at), (blocks,), jnp.float32, least / len(split), largest / len(split))
        loudness = loudness * jnp.repeat(jnp.exp(draws), extent[axis_at] // blocks).reshape((-1,) + (1,) * (len(extent) - 1 - axis_at))
    return loudness


def normal_values(own_key, dims, spread, limit, split=(), held_as=jnp.bfloat16):
    values = spread * jax.random.normal(own_key, dims, jnp.float32)
    if split:
        values = values * shard_levels(own_key, dims, split, -0.22, 0.18)
    return jnp.clip(values, -limit, limit).astype(held_as)


def setup_inputs(seed: int = 0) -> dict:
    keys = jax.random.split(jax.random.key(seed), 5)
    return {
        "fields": normal_values(keys[0], (BATCH, LATS, LONS, CHANNELS), 1.0, 6.0, ((0, 2), (1, 16))),
        "cotangent": normal_values(keys[1], (BATCH, LATS, LONS, CHANNELS), 1.0, 6.0, ((0, 2), (1, 16))),
        "weights": normal_values(keys[2], (DEGREES, 2, CHANNELS, CHANNELS), (2 * CHANNELS) ** -0.5, 0.21875, ((0, 16),)),
        "degree_of": jax.random.permutation(keys[3], DEGREES).astype(jnp.int32),
    }


def legendre_table(order_ids, lat_count, degree_count):
    colatitude = jnp.pi * (jnp.arange(lat_count, dtype=jnp.float32) + 0.5) / lat_count
    cosine = jnp.cos(colatitude)[None, :]
    log_sine = jnp.log(jnp.sin(colatitude))[None, :]
    order_col = order_ids.astype(jnp.int32)[:, None]
    order_real = order_col.astype(jnp.float32)
    steps_up = jnp.arange(1, degree_count + 1, dtype=jnp.float32)[None, :]
    factor = jnp.where(steps_up <= order_real, 0.5 * jnp.log((2.0 * steps_up + 1.0) / (2.0 * steps_up)), 0.0)
    log_start = 0.5 * jnp.log(1.0 / (4.0 * jnp.pi)) + lax.optimization_barrier(jnp.sum(factor, axis=1, keepdims=True))
    diagonal = jnp.exp(log_start + order_real * log_sine)
    squared = order_real * order_real

    def advance(carry, degree):
        previous, older = carry
        degree_real = degree.astype(jnp.float32)
        lead = jnp.sqrt(jnp.maximum(4.0 * degree_real * degree_real - 1.0, 0.0) / jnp.maximum(degree_real * degree_real - squared, 1.0))
        lower = degree_real - 1.0
        back = jnp.sqrt(jnp.maximum(lower * lower - squared, 0.0) / jnp.maximum(4.0 * lower * lower - 1.0, 1.0))
        general = lead * (cosine * previous - back * older)
        first = jnp.sqrt(2.0 * order_real + 3.0) * cosine * previous
        value = jnp.where(degree == order_col, diagonal, jnp.where(degree == order_col + 1, first, jnp.where(degree > order_col + 1, general, 0.0)))
        return ((value, previous), value)
    zeros = jnp.zeros((order_ids.shape[0], lat_count), jnp.float32)
    final_state, table = lax.scan(advance, (zeros, zeros), jnp.arange(degree_count, dtype=jnp.int32))
    return jnp.transpose(table, (1, 0, 2))

def spectral_tables(order_ids, degree_of, lat_count, degree_count):
    table = legendre_table(order_ids, lat_count, degree_count)
    chosen = jnp.take(table, degree_of.astype(jnp.int32), axis=1)
    colatitude = jnp.pi * (jnp.arange(lat_count, dtype=jnp.float32) + 0.5) / lat_count
    quadrature = 2.0 * jnp.pi * jnp.pi / lat_count * jnp.sin(colatitude)
    return ((chosen * quadrature[None, None, :]).astype(jnp.bfloat16), chosen.astype(jnp.bfloat16))

def fourier_tables(lon_count, order_count):
    lon_ids = jnp.arange(lon_count, dtype=jnp.int32)[:, None]
    order_ids = jnp.arange(order_count, dtype=jnp.int32)[None, :]
    phase = 2.0 * jnp.pi * (lon_ids * order_ids % lon_count).astype(jnp.float32) / lon_count
    forward = jnp.stack([jnp.cos(phase), -jnp.sin(phase)], axis=2).reshape(lon_count, 2 * order_count) / lon_count
    doubled = jnp.where(order_ids == 0, 1.0, 2.0)
    inverse = jnp.stack([doubled * jnp.cos(phase), -doubled * jnp.sin(phase)], axis=2).reshape(lon_count, 2 * order_count)
    return (forward.astype(jnp.bfloat16), jnp.transpose(inverse).astype(jnp.bfloat16))

def as_real(values):
    return values.astype(jnp.float32)

def sample_pass(field, cotangent, weights, forward, inverse, qslot, pslot):
    w_real = as_real(weights[:, 0])
    w_imag = as_real(weights[:, 1])
    spectra = jnp.einsum('ikc,kf->ifc', as_real(field), as_real(forward)).astype(jnp.bfloat16)
    spectra = spectra.reshape(LATS, ORDERS, 2, CHANNELS)
    coeffs = jnp.einsum('mji,imrc->jmrc', as_real(qslot), as_real(spectra)).astype(jnp.bfloat16)
    c_real = as_real(coeffs[:, :, 0])
    c_imag = as_real(coeffs[:, :, 1])
    f_real = jnp.einsum('jmc,jcd->jmd', c_real, w_real) - jnp.einsum('jmc,jcd->jmd', c_imag, w_imag)
    f_imag = jnp.einsum('jmc,jcd->jmd', c_real, w_imag) + jnp.einsum('jmc,jcd->jmd', c_imag, w_real)
    filtered = jnp.stack([f_real, f_imag], axis=2).astype(jnp.bfloat16)
    synth = jnp.einsum('mji,jmrc->imrc', as_real(pslot), as_real(filtered)).astype(jnp.bfloat16)
    response = jnp.einsum('ifc,fk->ikc', as_real(synth.reshape(LATS, 2 * ORDERS, CHANNELS)), as_real(inverse))
    activated, pullback = jax.vjp(jax.nn.gelu, response)
    upstream = pullback(as_real(cotangent))[0].astype(jnp.bfloat16)
    grad_synth = jnp.einsum('ikc,fk->ifc', as_real(upstream), as_real(inverse)).astype(jnp.bfloat16)
    grad_synth = grad_synth.reshape(LATS, ORDERS, 2, CHANNELS)
    grad_filtered = jnp.einsum('mji,imrc->jmrc', as_real(pslot), as_real(grad_synth)).astype(jnp.bfloat16)
    g_real = as_real(grad_filtered[:, :, 0])
    g_imag = as_real(grad_filtered[:, :, 1])
    dw_real = jnp.einsum('jmc,jmd->jcd', c_real, g_real) + jnp.einsum('jmc,jmd->jcd', c_imag, g_imag)
    dw_imag = jnp.einsum('jmc,jmd->jcd', c_real, g_imag) - jnp.einsum('jmc,jmd->jcd', c_imag, g_real)
    a_real = jnp.einsum('jmd,jcd->jmc', g_real, w_real) + jnp.einsum('jmd,jcd->jmc', g_imag, w_imag)
    a_imag = jnp.einsum('jmd,jcd->jmc', g_imag, w_real) - jnp.einsum('jmd,jcd->jmc', g_real, w_imag)
    grad_coeffs = jnp.stack([a_real, a_imag], axis=2).astype(jnp.bfloat16)
    grad_spectra = jnp.einsum('mji,jmrc->imrc', as_real(qslot), as_real(grad_coeffs)).astype(jnp.bfloat16)
    delta = jnp.einsum('ifc,kf->ikc', as_real(grad_spectra.reshape(LATS, 2 * ORDERS, CHANNELS)), as_real(forward))
    grad_field = (as_real(cotangent) + delta).astype(jnp.bfloat16)
    return (grad_field, jnp.stack([dw_real, dw_imag], axis=1))

def reference(fields, cotangent, weights, degree_of):
    forward, inverse = fourier_tables(LONS, ORDERS)
    qslot, pslot = spectral_tables(jnp.arange(ORDERS, dtype=jnp.int32), degree_of, LATS, DEGREES)

    def one_sample(total, pair):
        grad_field, weight_part = sample_pass(pair[0], pair[1], weights, forward, inverse, qslot, pslot)
        return (total + weight_part, grad_field)
    start = jnp.zeros((DEGREES, 2, CHANNELS, CHANNELS), jnp.float32)
    total, grad_fields = lax.scan(one_sample, start, (fields, cotangent))
    return (grad_fields, total.astype(jnp.bfloat16))
```

```python
import jax
import jax.numpy as jnp
from jax import lax
from jax.experimental import pallas as pl
from jax.experimental.pallas import tpu as pltpu
from jax.sharding import PartitionSpec as P

LATS = 192
LONS = 384
ORDERS = 128
DEGREES = 128
CHANNELS = 384
LANES = 128


def table_kernel(deg_ref, diag_ref, cos_ref, quad_ref, order_ref, q_ref, p_ref, slot_ref, rows_ref):
    orders = diag_ref.shape[0]
    lats = q_ref.shape[2]
    degrees = deg_ref.shape[0]

    def invert(slot, carry):
        slot_ref[deg_ref[slot]] = slot
        return carry

    lax.fori_loop(0, degrees, invert, 0)
    order_real = order_ref[...]
    squared = order_real * order_real
    diagonal = diag_ref[...]
    cosine = cos_ref[...]
    first_lead = jnp.sqrt(2.0 * order_real + 3.0)
    halves = rows_ref.shape[0]

    def advance(degree, carry):
        previous, older = carry
        degree_real = degree.astype(jnp.float32)
        lead = jnp.sqrt(
            jnp.maximum(4.0 * degree_real * degree_real - 1.0, 0.0)
            / jnp.maximum(degree_real * degree_real - squared, 1.0)
        )
        lower = degree_real - 1.0
        back = jnp.sqrt(
            jnp.maximum(lower * lower - squared, 0.0) / jnp.maximum(4.0 * lower * lower - 1.0, 1.0)
        )
        general = lead * (cosine * previous - back * older)
        first = first_lead * cosine * previous
        value = jnp.where(
            degree_real == order_real,
            diagonal,
            jnp.where(
                degree_real == order_real + 1.0,
                first,
                jnp.where(degree_real > order_real + 1.0, general, 0.0),
            ),
        )
        slot = slot_ref[degree]
        for half in range(halves):
            rows_ref[half, pl.ds(slot, orders, stride=degrees), :] = value[
                :, half * LANES : (half + 1) * LANES
            ]
        return (value, previous)

    zeros = diagonal * 0.0
    lax.fori_loop(0, degrees, advance, (zeros, zeros), unroll=4)
    quadrature = quad_ref[...]
    for order in range(orders):
        for half in range(halves):
            low = half * LANES
            high = min(lats, low + LANES)
            chosen = rows_ref[half, order * degrees : (order + 1) * degrees, :][:, : high - low]
            p_ref[order, :, low:high] = chosen.astype(jnp.bfloat16)
            q_ref[order, :, low:high] = (chosen * quadrature[:, low:high]).astype(jnp.bfloat16)


def spectral_tables(start, ord_dev, degree_of):
    halves = -(-LATS // LANES)
    padded = halves * LANES
    order_col = (start + jnp.arange(ord_dev, dtype=jnp.int32)).astype(jnp.float32)[:, None]
    lat_ids = jnp.minimum(jnp.arange(padded, dtype=jnp.float32), LATS - 1.0)
    colatitude = jnp.pi * (lat_ids + 0.5) / LATS
    sine = jnp.sin(colatitude)[None, :]
    steps_up = jnp.arange(1, DEGREES + 1, dtype=jnp.float32)[None, :]
    factor = jnp.where(
        steps_up <= order_col, 0.5 * jnp.log((2.0 * steps_up + 1.0) / (2.0 * steps_up)), 0.0
    )
    log_start = 0.5 * jnp.log(1.0 / (4.0 * jnp.pi)) + jnp.sum(factor, axis=1, keepdims=True)
    diagonal = jnp.exp(log_start + order_col * jnp.log(sine))
    cosine = jnp.broadcast_to(jnp.cos(colatitude)[None, :], diagonal.shape)
    quadrature = 2.0 * jnp.pi * jnp.pi / LATS * sine
    orders = jnp.broadcast_to(order_col, diagonal.shape)
    vmem = pl.BlockSpec(memory_space=pltpu.VMEM)
    shape = jax.ShapeDtypeStruct((ord_dev, DEGREES, LATS), jnp.bfloat16)
    return pl.pallas_call(
        table_kernel,
        out_shape=(shape, shape),
        in_specs=[pl.BlockSpec(memory_space=pltpu.SMEM)] + [vmem] * 4,
        out_specs=(vmem, vmem),
        scratch_shapes=[
            pltpu.SMEM((DEGREES,), jnp.int32),
            pltpu.VMEM((halves, ord_dev * DEGREES, LANES), jnp.float32),
        ],
        name="legendre_tables",
    )(degree_of, diagonal, cosine, quadrature, orders)


def fourier_tables(lon_count, order_count):
    lon_ids = jnp.arange(lon_count, dtype=jnp.int32)[:, None]
    order_ids = jnp.arange(order_count, dtype=jnp.int32)[None, :]
    phase = 2.0 * jnp.pi * (lon_ids * order_ids % lon_count).astype(jnp.float32) / lon_count
    forward = (
        jnp.stack([jnp.cos(phase), -jnp.sin(phase)], axis=2).reshape(lon_count, 2 * order_count)
        / lon_count
    )
    doubled = jnp.where(order_ids == 0, 1.0, 2.0)
    inverse = jnp.stack([doubled * jnp.cos(phase), -doubled * jnp.sin(phase)], axis=2).reshape(
        lon_count, 2 * order_count
    )
    return (forward.astype(jnp.bfloat16), jnp.transpose(inverse).astype(jnp.bfloat16))


def to_orders(values):
    return lax.all_to_all(values, "lat", split_axis=1, concat_axis=0, tiled=True)


def to_degrees(values):
    return lax.all_to_all(values, "lat", split_axis=0, concat_axis=1, tiled=True)


def back_to_orders(values):
    return lax.all_to_all(values, "lat", split_axis=1, concat_axis=0, tiled=True)


def to_bands(values):
    return lax.all_to_all(values, "lat", split_axis=0, concat_axis=1, tiled=True)


def product(spec, left, right):
    return jnp.einsum(spec, left, right, preferred_element_type=jnp.float32)


def apply_filter(coeffs, weights):
    c_real = coeffs[:, :, 0]
    c_imag = coeffs[:, :, 1]
    w_real = weights[:, 0]
    w_imag = weights[:, 1]
    f_real = product("jmsc,jcd->jmsd", c_real, w_real) - product("jmsc,jcd->jmsd", c_imag, w_imag)
    f_imag = product("jmsc,jcd->jmsd", c_real, w_imag) + product("jmsc,jcd->jmsd", c_imag, w_real)
    return jnp.stack([f_real, f_imag], axis=2).astype(jnp.bfloat16)


def adjoint_filter(grads, weights):
    g_real = grads[:, :, 0]
    g_imag = grads[:, :, 1]
    w_real = weights[:, 0]
    w_imag = weights[:, 1]
    a_real = product("jmsd,jcd->jmsc", g_real, w_real) + product("jmsd,jcd->jmsc", g_imag, w_imag)
    a_imag = product("jmsd,jcd->jmsc", g_imag, w_real) - product("jmsd,jcd->jmsc", g_real, w_imag)
    return jnp.stack([a_real, a_imag], axis=2).astype(jnp.bfloat16)


def filter_grad(coeffs, grads):
    c_real = coeffs[:, :, 0]
    c_imag = coeffs[:, :, 1]
    g_real = grads[:, :, 0]
    g_imag = grads[:, :, 1]
    dw_real = product("jmsc,jmsd->jcd", c_real, g_real) + product("jmsc,jmsd->jcd", c_imag, g_imag)
    dw_imag = product("jmsc,jmsd->jcd", c_real, g_imag) - product("jmsc,jmsd->jcd", c_imag, g_real)
    return jnp.stack([dw_real, dw_imag], axis=1)


def local(fields, cotangent, weights, degree_of):
    samples = fields.shape[0]
    band_rows = fields.shape[1]
    ord_dev = ORDERS // lax.axis_size("lat")
    forward, inverse = fourier_tables(LONS, ORDERS)
    qslot, pslot = spectral_tables(lax.axis_index("lat") * ord_dev, ord_dev, degree_of)
    spectra = product("sikc,kf->ifsc", fields, forward).astype(jnp.bfloat16)
    spectra = spectra.reshape(band_rows, ORDERS, 2, samples, CHANNELS)
    gathered = to_orders(spectra)
    coeffs_local = product("mji,imrsc->jmrsc", qslot, gathered).astype(jnp.bfloat16)
    coeffs = to_degrees(coeffs_local)
    filtered = apply_filter(coeffs, weights)
    returned = back_to_orders(filtered)
    synth_local = product("mji,jmrsc->imrsc", pslot, returned).astype(jnp.bfloat16)
    synth = to_bands(synth_local)
    response = product(
        "ifsc,fk->sikc", synth.reshape(band_rows, 2 * ORDERS, samples, CHANNELS), inverse
    )
    activated, pullback = jax.vjp(jax.nn.gelu, response)
    upstream = pullback(cotangent.astype(jnp.float32))[0].astype(jnp.bfloat16)
    grad_synth = product("sikc,fk->ifsc", upstream, inverse).astype(jnp.bfloat16)
    grad_synth = grad_synth.reshape(band_rows, ORDERS, 2, samples, CHANNELS)
    grad_gathered = to_orders(grad_synth)
    grad_local = product("mji,imrsc->jmrsc", pslot, grad_gathered).astype(jnp.bfloat16)
    grad_filtered = to_degrees(grad_local)
    weight_total = lax.psum(filter_grad(coeffs, grad_filtered).astype(jnp.bfloat16), "batch")
    grad_coeffs = adjoint_filter(grad_filtered, weights)
    grad_back = back_to_orders(grad_coeffs)
    grad_local_spec = product("mji,jmrsc->imrsc", qslot, grad_back).astype(jnp.bfloat16)
    grad_bands = to_bands(grad_local_spec)
    delta = product(
        "ifsc,kf->sikc", grad_bands.reshape(band_rows, 2 * ORDERS, samples, CHANNELS), forward
    )
    grad_fields = (cotangent.astype(jnp.float32) + delta).astype(jnp.bfloat16)
    return (grad_fields, weight_total)


def solution(mesh):
    return jax.shard_map(
        local,
        mesh=mesh,
        in_specs=(
            P("batch", "lat", None, None),
            P("batch", "lat", None, None),
            P("lat", None, None, None),
            P(),
        ),
        out_specs=(P("batch", "lat", None, None), P("lat", None, None, None)),
        check_vma=False,
    )
```

```python
import functools

import jax
import jax.numpy as jnp
from jax import lax
from jax.experimental import pallas as pl
from jax.experimental.pallas import tpu as pltpu
from jax.sharding import PartitionSpec as P

LATS = 192
LONS = 384
ORDERS = 128
DEGREES = 128
CHANNELS = 384
LANES = 128


def table_kernel(deg_ref, diag_ref, cos_ref, quad_ref, order_ref, q_ref, p_ref, slot_ref, rows_ref):
    orders = diag_ref.shape[0]
    lats = q_ref.shape[2]
    degrees = deg_ref.shape[0]

    def invert(slot, carry):
        slot_ref[deg_ref[slot]] = slot
        return carry

    lax.fori_loop(0, degrees, invert, 0)
    order_real = order_ref[...]
    squared = order_real * order_real
    diagonal = diag_ref[...]
    cosine = cos_ref[...]
    first_lead = jnp.sqrt(2.0 * order_real + 3.0)
    halves = rows_ref.shape[0]

    def advance(degree, carry):
        previous, older = carry
        degree_real = degree.astype(jnp.float32)
        lead = jnp.sqrt(
            jnp.maximum(4.0 * degree_real * degree_real - 1.0, 0.0)
            / jnp.maximum(degree_real * degree_real - squared, 1.0)
        )
        lower = degree_real - 1.0
        back = jnp.sqrt(
            jnp.maximum(lower * lower - squared, 0.0) / jnp.maximum(4.0 * lower * lower - 1.0, 1.0)
        )
        general = lead * (cosine * previous - back * older)
        first = first_lead * cosine * previous
        value = jnp.where(
            degree_real == order_real,
            diagonal,
            jnp.where(
                degree_real == order_real + 1.0,
                first,
                jnp.where(degree_real > order_real + 1.0, general, 0.0),
            ),
        )
        slot = slot_ref[degree]
        for half in range(halves):
            rows_ref[half, pl.ds(slot, orders, stride=degrees), :] = value[
                :, half * LANES : (half + 1) * LANES
            ]
        return (value, previous)

    zeros = diagonal * 0.0
    lax.fori_loop(0, degrees, advance, (zeros, zeros), unroll=4)
    quadrature = quad_ref[...]
    for order in range(orders):
        for half in range(halves):
            low = half * LANES
            high = min(lats, low + LANES)
            chosen = rows_ref[half, order * degrees : (order + 1) * degrees, :][:, : high - low]
            p_ref[order, :, low:high] = chosen.astype(jnp.bfloat16)
            q_ref[order, :, low:high] = (chosen * quadrature[:, low:high]).astype(jnp.bfloat16)


def spectral_tables(start, ord_dev, degree_of):
    halves = -(-LATS // LANES)
    padded = halves * LANES
    order_col = (start + jnp.arange(ord_dev, dtype=jnp.int32)).astype(jnp.float32)[:, None]
    lat_ids = jnp.minimum(jnp.arange(padded, dtype=jnp.float32), LATS - 1.0)
    colatitude = jnp.pi * (lat_ids + 0.5) / LATS
    sine = jnp.sin(colatitude)[None, :]
    steps_up = jnp.arange(1, DEGREES + 1, dtype=jnp.float32)[None, :]
    factor = jnp.where(
        steps_up <= order_col, 0.5 * jnp.log((2.0 * steps_up + 1.0) / (2.0 * steps_up)), 0.0
    )
    log_start = 0.5 * jnp.log(1.0 / (4.0 * jnp.pi)) + jnp.sum(factor, axis=1, keepdims=True)
    diagonal = jnp.exp(log_start + order_col * jnp.log(sine))
    cosine = jnp.broadcast_to(jnp.cos(colatitude)[None, :], diagonal.shape)
    quadrature = 2.0 * jnp.pi * jnp.pi / LATS * sine
    orders = jnp.broadcast_to(order_col, diagonal.shape)
    vmem = pl.BlockSpec(memory_space=pltpu.VMEM)
    shape = jax.ShapeDtypeStruct((ord_dev, DEGREES, LATS), jnp.bfloat16)
    return pl.pallas_call(
        table_kernel,
        out_shape=(shape, shape),
        in_specs=[pl.BlockSpec(memory_space=pltpu.SMEM)] + [vmem] * 4,
        out_specs=(vmem, vmem),
        scratch_shapes=[
            pltpu.SMEM((DEGREES,), jnp.int32),
            pltpu.VMEM((halves, ord_dev * DEGREES, LANES), jnp.float32),
        ],
        name="legendre_tables",
    )(degree_of, diagonal, cosine, quadrature, orders)


def fourier_tables(lon_count, order_count):
    lon_ids = jnp.arange(lon_count, dtype=jnp.int32)[:, None]
    order_ids = jnp.arange(order_count, dtype=jnp.int32)[None, :]
    phase = 2.0 * jnp.pi * (lon_ids * order_ids % lon_count).astype(jnp.float32) / lon_count
    forward = (
        jnp.stack([jnp.cos(phase), -jnp.sin(phase)], axis=2).reshape(lon_count, 2 * order_count)
        / lon_count
    )
    doubled = jnp.where(order_ids == 0, 1.0, 2.0)
    inverse = jnp.stack([doubled * jnp.cos(phase), -doubled * jnp.sin(phase)], axis=2).reshape(
        lon_count, 2 * order_count
    )
    return (forward.astype(jnp.bfloat16), jnp.transpose(inverse).astype(jnp.bfloat16))


def to_orders(values):
    return lax.all_to_all(values, "lat", split_axis=1, concat_axis=0, tiled=True)


def to_degrees(values):
    return lax.all_to_all(values, "lat", split_axis=0, concat_axis=1, tiled=True)


def back_to_orders(values):
    return lax.all_to_all(values, "lat", split_axis=1, concat_axis=0, tiled=True)


def to_bands(values):
    return lax.all_to_all(values, "lat", split_axis=0, concat_axis=1, tiled=True)


def product(spec, left, right):
    return jnp.einsum(spec, left, right, preferred_element_type=jnp.float32)


def apply_filter(coeffs, weights):
    c_real = coeffs[:, :, 0]
    c_imag = coeffs[:, :, 1]
    w_real = weights[:, 0]
    w_imag = weights[:, 1]
    f_real = product("jmsc,jcd->jmsd", c_real, w_real) - product("jmsc,jcd->jmsd", c_imag, w_imag)
    f_imag = product("jmsc,jcd->jmsd", c_real, w_imag) + product("jmsc,jcd->jmsd", c_imag, w_real)
    return jnp.stack([f_real, f_imag], axis=2).astype(jnp.bfloat16)


def adjoint_filter(grads, weights):
    g_real = grads[:, :, 0]
    g_imag = grads[:, :, 1]
    w_real = weights[:, 0]
    w_imag = weights[:, 1]
    a_real = product("jmsd,jcd->jmsc", g_real, w_real) + product("jmsd,jcd->jmsc", g_imag, w_imag)
    a_imag = product("jmsd,jcd->jmsc", g_imag, w_real) - product("jmsd,jcd->jmsc", g_real, w_imag)
    return jnp.stack([a_real, a_imag], axis=2).astype(jnp.bfloat16)


def filter_grad(coeffs, grads):
    c_real = coeffs[:, :, 0]
    c_imag = coeffs[:, :, 1]
    g_real = grads[:, :, 0]
    g_imag = grads[:, :, 1]
    dw_real = product("jmsc,jmsd->jcd", c_real, g_real) + product("jmsc,jmsd->jcd", c_imag, g_imag)
    dw_imag = product("jmsc,jmsd->jcd", c_real, g_imag) - product("jmsc,jmsd->jcd", c_imag, g_real)
    return jnp.stack([dw_real, dw_imag], axis=1)


def pair_swap(values, even_sign):
    rows = values.shape[0]
    even = lax.broadcasted_iota(jnp.int32, values.shape, 0) % 2 == 0
    above = pltpu.roll(values, rows - 1, 0)
    below = pltpu.roll(values, 1, 0)
    return jnp.where(even, even_sign * above, -even_sign * below)


def gelu_slope(x):
    scale = 0.7978845608028654
    square = x * x
    t = jnp.tanh(scale * (x + 0.044715 * x * square))
    return 0.5 * (1.0 + t) + 0.5 * x * (1.0 - t * t) * (scale * (1.0 + 0.134145 * square))


def dot(left, right, dims=((1,), (0,))):
    return lax.dot_general(left, right, (dims, ((), ())), preferred_element_type=jnp.float32)


def block_kernel(
    n, nb, fields, cotangent, weights, qtab, ptab, fwd_fk, fwd_kf, inv_fk, inv_kf,
    grad_out, dw_out,
    fbuf, cbuf, wbuf, band_out, band_in, ord_in, ord_out, deg_out, deg_back, co, go, mixed,
    wide_a, wide_b, dw, dw_in,
    load_sem, send_sem, recv_sem, dw_send, dw_recv, out_sem,
):
    me = lax.axis_index("lat")
    me_b = lax.axis_index("batch")
    chunks, lat_dev = fbuf.shape[0], fbuf.shape[1]
    orders = qtab.shape[0]
    rows = 2 * orders
    slots = co.shape[1]
    degrees = n * slots
    lats = n * lat_dev
    mesh_id = pl.DeviceIdType.MESH

    def lanes(chunk):
        return pl.ds(chunk * LANES, LANES)

    def load(chunk):
        return pltpu.make_async_copy(
            fields.at[0, :, :, lanes(chunk)], fbuf.at[chunk], load_sem.at[chunk]
        )

    def load_cot(chunk):
        return pltpu.make_async_copy(
            cotangent.at[0, :, :, lanes(chunk)], cbuf.at[chunk], load_sem.at[chunks + chunk]
        )

    load_w = pltpu.make_async_copy(weights, wbuf, load_sem.at[2 * chunks])
    for chunk in range(chunks):
        load(chunk).start()
    load_w.start()
    for chunk in range(chunks):
        load_cot(chunk).start()

    barrier = pltpu.get_barrier_semaphore()

    def greet(step, carry):
        peer = lax.rem(me + step, n)
        pl.semaphore_signal(barrier, inc=1, device_id={"lat": peer}, device_id_type=mesh_id)
        return carry

    lax.fori_loop(1, n, greet, 0)
    for step in range(1, nb):
        peer = lax.rem(me_b + step, nb)
        pl.semaphore_signal(barrier, inc=1, device_id={"batch": peer}, device_id_type=mesh_id)
    pl.semaphore_wait(barrier, n - 1 + nb - 1)

    def part(ref, chunk, kind, owner):
        if kind == "band":
            return ref.at[chunk, :, pl.ds(pl.multiple_of(owner * rows, rows), rows), :]
        if kind == "lat":
            return ref.at[chunk, pl.ds(owner * lat_dev, lat_dev)]
        return ref.at[chunk, pl.ds(owner * slots, slots)]

    def exchange(stage, chunk, source, source_kind, target, target_kind):
        def send(step, carry):
            peer = lax.rem(me + step, n)
            pltpu.make_async_remote_copy(
                src_ref=part(source, chunk, source_kind, peer),
                dst_ref=part(target, chunk, target_kind, me),
                send_sem=send_sem.at[stage, chunk],
                recv_sem=recv_sem.at[stage, chunk],
                device_id={"lat": peer},
                device_id_type=mesh_id,
            ).start()
            return carry

        lax.fori_loop(1, n, send, 0)
        pltpu.make_async_copy(
            part(source, chunk, source_kind, me),
            part(target, chunk, target_kind, me),
            recv_sem.at[stage, chunk],
        ).start()

    def arrived(stage, chunk, target):
        pltpu.make_async_copy(target.at[chunk], target.at[chunk], recv_sem.at[stage, chunk]).wait()

    def departed(stage, chunk, source, kind):
        if kind == "band":
            view = source.at[chunk, :, 0 : (n - 1) * rows, :]
        elif kind == "lat":
            view = source.at[chunk, 0 : (n - 1) * lat_dev]
        else:
            view = source.at[chunk, 0 : (n - 1) * slots]
        pltpu.make_async_copy(view, view, send_sem.at[stage, chunk]).wait()

    def widen(source, chunk, depth):
        def one(block, carry):
            piece = source[chunk, pl.ds(block * depth, depth)].astype(jnp.float32)
            wide_a[pl.ds(pl.multiple_of(block * depth * rows, depth * rows), depth * rows), :] = (
                piece.reshape(depth * rows, LANES)
            )
            return carry

        lax.fori_loop(0, n, one, 0)

    def narrow(target, chunk, depth):
        def one(block, carry):
            start = pl.multiple_of(block * depth * rows, depth * rows)
            piece = wide_b[pl.ds(start, depth * rows), :]
            target[chunk, pl.ds(block * depth, depth)] = piece.reshape(
                depth, rows, LANES
            ).astype(jnp.bfloat16)
            return carry

        lax.fori_loop(0, n, one, 0)

    def apply_table(table, depth_in, depth_out, dims):
        def one(order, carry):
            real = wide_a[pl.ds(2 * order, depth_in, stride=rows), :]
            imag = wide_a[pl.ds(2 * order + 1, depth_in, stride=rows), :]
            both = jnp.concatenate([real, imag], axis=1).astype(jnp.bfloat16)
            result = dot(table[order], both, dims)
            wide_b[pl.ds(2 * order, depth_out, stride=rows), :] = result[:, :LANES]
            wide_b[pl.ds(2 * order + 1, depth_out, stride=rows), :] = result[:, LANES:]
            return carry

        lax.fori_loop(0, orders, one, 0)

    def analyse(stage, chunk, table, target, before):
        arrived(stage, chunk, ord_in)
        widen(ord_in, chunk, lat_dev)
        apply_table(table, lats, degrees, ((1,), (0,)))
        if before is not None:
            departed(before, chunk, deg_out, "slot")
        narrow(deg_out, chunk, slots)
        exchange(stage + 1, chunk, deg_out, "slot", target, "band")

    def synthesise(stage, chunk, table, before):
        arrived(stage, chunk, deg_back)
        widen(deg_back, chunk, slots)
        apply_table(table, degrees, lats, ((0,), (0,)))
        if before is not None:
            departed(before, chunk, ord_out, "lat")
        narrow(ord_out, chunk, lat_dev)
        exchange(stage + 1, chunk, ord_out, "lat", band_in, "band")

    def joined(source, slot):
        return jnp.concatenate([source[chunk, slot] for chunk in range(chunks)], axis=1)

    for chunk in range(chunks):
        load(chunk).wait()

        def fourier(row, carry):
            band_out[chunk, row] = dot(fwd_fk[...], fbuf[chunk, row]).astype(jnp.bfloat16)
            return carry

        lax.fori_loop(0, lat_dev, fourier, 0)
        exchange(0, chunk, band_out, "band", ord_in, "lat")
    for chunk in range(chunks):
        analyse(0, chunk, qtab, co, None)
    load_w.wait()
    for chunk in range(chunks):
        arrived(1, chunk, co)
    for chunk in range(chunks):

        def mix(slot, carry):
            values = joined(co, slot)
            same = dot(values, wbuf[slot, 0, :, chunk * LANES : (chunk + 1) * LANES])
            cross = dot(values, wbuf[slot, 1, :, chunk * LANES : (chunk + 1) * LANES])
            mixed[chunk, slot] = (same + pair_swap(cross, -1.0)).astype(jnp.bfloat16)
            return carry

        lax.fori_loop(0, slots, mix, 0)
        exchange(2, chunk, mixed, "band", deg_back, "slot")
    for chunk in range(chunks):
        synthesise(2, chunk, ptab, None)
    for chunk in range(chunks):
        load_cot(chunk).wait()
        arrived(3, chunk, band_in)
        departed(0, chunk, band_out, "band")

        def middle(row, carry):
            response = dot(inv_kf[...], band_in[chunk, row])
            upstream = cbuf[chunk, row].astype(jnp.float32) * gelu_slope(response)
            band_out[chunk, row] = dot(inv_fk[...], upstream.astype(jnp.bfloat16)).astype(
                jnp.bfloat16
            )
            return carry

        lax.fori_loop(0, lat_dev, middle, 0)
        exchange(4, chunk, band_out, "band", ord_in, "lat")
    for chunk in range(chunks):
        analyse(4, chunk, ptab, go, 1)
    for chunk in range(chunks):
        arrived(5, chunk, go)
    for chunk in range(chunks):
        departed(2, chunk, mixed, "band")

        def adjoint(slot, carry):
            values = joined(go, slot)
            span = ((1,), (1,))
            same = dot(values, wbuf[slot, 0, chunk * LANES : (chunk + 1) * LANES, :], span)
            cross = dot(values, wbuf[slot, 1, chunk * LANES : (chunk + 1) * LANES, :], span)
            mixed[chunk, slot] = (same + pair_swap(cross, 1.0)).astype(jnp.bfloat16)
            return carry

        lax.fori_loop(0, slots, adjoint, 0)
        exchange(6, chunk, mixed, "band", deg_back, "slot")

    def weight_grad(slot, carry):
        values = joined(co, slot)
        grads = joined(go, slot)
        turned = pair_swap(grads.astype(jnp.float32), 1.0).astype(jnp.bfloat16)
        span = ((0,), (0,))
        dw[slot, 0] = dot(values, grads, span).astype(jnp.bfloat16)
        dw[slot, 1] = dot(values, turned, span).astype(jnp.bfloat16)
        return carry

    lax.fori_loop(0, slots, weight_grad, 0)
    dw_copies = []
    for step in range(1, nb):
        peer = lax.rem(me_b + step, nb)
        copy = pltpu.make_async_remote_copy(
            src_ref=dw,
            dst_ref=dw_in.at[step - 1],
            send_sem=dw_send.at[step - 1],
            recv_sem=dw_recv.at[step - 1],
            device_id={"batch": peer},
            device_id_type=mesh_id,
        )
        copy.start()
        dw_copies.append(copy)
    for chunk in range(chunks):
        synthesise(6, chunk, qtab, 3)
    for copy in dw_copies:
        copy.wait()

    def total(slot, carry):
        value = dw[slot].astype(jnp.float32)
        for step in range(nb - 1):
            value = value + dw_in[step, slot].astype(jnp.float32)
        dw[slot] = value.astype(jnp.bfloat16)
        return carry

    lax.fori_loop(0, slots, total, 0)
    store_w = pltpu.make_async_copy(dw, dw_out, out_sem.at[chunks])
    store_w.start()

    def store(chunk):
        return pltpu.make_async_copy(
            cbuf.at[chunk], grad_out.at[0, :, :, lanes(chunk)], out_sem.at[chunk]
        )

    for chunk in range(chunks):
        arrived(7, chunk, band_in)

        def finish(row, carry):
            delta = dot(fwd_kf[...], band_in[chunk, row])
            cbuf[chunk, row] = (cbuf[chunk, row].astype(jnp.float32) + delta).astype(jnp.bfloat16)
            return carry

        lax.fori_loop(0, lat_dev, finish, 0)
        store(chunk).start()
    for chunk in range(chunks):
        departed(4, chunk, band_out, "band")
        departed(5, chunk, deg_out, "slot")
        departed(6, chunk, mixed, "band")
        departed(7, chunk, ord_out, "lat")
        store(chunk).wait()
    store_w.wait()


def local_kernel(fields, cotangent, weights, degree_of):
    if fields.shape[0] != 1:
        return local(fields, cotangent, weights, degree_of)
    n = lax.axis_size("lat")
    nb = lax.axis_size("batch")
    lat_dev, lons, channels = fields.shape[1:]
    slots = weights.shape[0]
    orders = ORDERS // n
    rows = 2 * orders
    chunks = channels // LANES
    forward, inverse = fourier_tables(LONS, ORDERS)
    qtab, ptab = spectral_tables(lax.axis_index("lat") * orders, orders, degree_of)
    vmem = pl.BlockSpec(memory_space=pltpu.VMEM)
    anywhere = pl.BlockSpec(memory_space=pl.ANY)

    def buffer(*dims):
        return pltpu.VMEM(dims, jnp.bfloat16)

    dma = pltpu.SemaphoreType.DMA
    others = max(nb - 1, 1)
    wide_rows = max(LATS, DEGREES) * rows
    return pl.pallas_call(
        functools.partial(block_kernel, n, nb),
        out_shape=(
            jax.ShapeDtypeStruct(fields.shape, jnp.bfloat16),
            jax.ShapeDtypeStruct(weights.shape, jnp.bfloat16),
        ),
        in_specs=[anywhere] * 3 + [vmem] * 6,
        out_specs=(anywhere, anywhere),
        scratch_shapes=[
            buffer(chunks, lat_dev, lons, LANES),
            buffer(chunks, lat_dev, lons, LANES),
            buffer(*weights.shape),
            buffer(chunks, lat_dev, n * rows, LANES),
            buffer(chunks, lat_dev, n * rows, LANES),
            buffer(chunks, LATS, rows, LANES),
            buffer(chunks, LATS, rows, LANES),
            buffer(chunks, DEGREES, rows, LANES),
            buffer(chunks, DEGREES, rows, LANES),
            buffer(chunks, slots, n * rows, LANES),
            buffer(chunks, slots, n * rows, LANES),
            buffer(chunks, slots, n * rows, LANES),
            pltpu.VMEM((wide_rows, LANES), jnp.float32),
            pltpu.VMEM((wide_rows, LANES), jnp.float32),
            buffer(*weights.shape),
            buffer(others, *weights.shape),
            dma((2 * chunks + 1,)),
            dma((8, chunks)),
            dma((8, chunks)),
            dma((others,)),
            dma((others,)),
            dma((chunks + 1,)),
        ],
        compiler_params=pltpu.CompilerParams(
            collective_id=0, has_side_effects=True, vmem_limit_bytes=60 * 2**20
        ),
        name="filter_block",
    )(
        fields, cotangent, weights, qtab, ptab,
        jnp.transpose(forward), forward, inverse, jnp.transpose(inverse),
    )


def local(fields, cotangent, weights, degree_of):
    samples = fields.shape[0]
    band_rows = fields.shape[1]
    ord_dev = ORDERS // lax.axis_size("lat")
    forward, inverse = fourier_tables(LONS, ORDERS)
    qslot, pslot = spectral_tables(lax.axis_index("lat") * ord_dev, ord_dev, degree_of)
    spectra = product("sikc,kf->ifsc", fields, forward).astype(jnp.bfloat16)
    spectra = spectra.reshape(band_rows, ORDERS, 2, samples, CHANNELS)
    gathered = to_orders(spectra)
    coeffs_local = product("mji,imrsc->jmrsc", qslot, gathered).astype(jnp.bfloat16)
    coeffs = to_degrees(coeffs_local)
    filtered = apply_filter(coeffs, weights)
    returned = back_to_orders(filtered)
    synth_local = product("mji,jmrsc->imrsc", pslot, returned).astype(jnp.bfloat16)
    synth = to_bands(synth_local)
    response = product(
        "ifsc,fk->sikc", synth.reshape(band_rows, 2 * ORDERS, samples, CHANNELS), inverse
    )
    activated, pullback = jax.vjp(jax.nn.gelu, response)
    upstream = pullback(cotangent.astype(jnp.float32))[0].astype(jnp.bfloat16)
    grad_synth = product("sikc,fk->ifsc", upstream, inverse).astype(jnp.bfloat16)
    grad_synth = grad_synth.reshape(band_rows, ORDERS, 2, samples, CHANNELS)
    grad_gathered = to_orders(grad_synth)
    grad_local = product("mji,imrsc->jmrsc", pslot, grad_gathered).astype(jnp.bfloat16)
    grad_filtered = to_degrees(grad_local)
    weight_total = lax.psum(filter_grad(coeffs, grad_filtered).astype(jnp.bfloat16), "batch")
    grad_coeffs = adjoint_filter(grad_filtered, weights)
    grad_back = back_to_orders(grad_coeffs)
    grad_local_spec = product("mji,jmrsc->imrsc", qslot, grad_back).astype(jnp.bfloat16)
    grad_bands = to_bands(grad_local_spec)
    delta = product(
        "ifsc,kf->sikc", grad_bands.reshape(band_rows, 2 * ORDERS, samples, CHANNELS), forward
    )
    grad_fields = (cotangent.astype(jnp.float32) + delta).astype(jnp.bfloat16)
    return (grad_fields, weight_total)


def solution(mesh):
    orders = ORDERS // mesh.shape["lat"]
    return jax.shard_map(
        local_kernel if orders % 8 == 0 and CHANNELS % LANES == 0 else local,
        mesh=mesh,
        in_specs=(
            P("batch", "lat", None, None),
            P("batch", "lat", None, None),
            P("lat", None, None, None),
            P(),
        ),
        out_specs=(P("batch", "lat", None, None), P("lat", None, None, None)),
        check_vma=False,
    )
```

```python
import functools

import jax
import numpy as np
import jax.numpy as jnp
from jax import lax
from jax.experimental import pallas as pl
from jax.experimental.pallas import tpu as pltpu
from jax.sharding import PartitionSpec as P

LATS = 192
LONS = 384
ORDERS = 128
DEGREES = 128
CHANNELS = 384
LANES = 128


def table_kernel(deg_ref, diag_ref, cos_ref, quad_ref, order_ref, q_ref, p_ref, slot_ref, rows_ref):
    orders = diag_ref.shape[0]
    lats = q_ref.shape[2]
    degrees = deg_ref.shape[0]

    def invert(slot, carry):
        slot_ref[deg_ref[slot]] = slot
        return carry

    lax.fori_loop(0, degrees, invert, 0)
    order_real = order_ref[...]
    squared = order_real * order_real
    diagonal = diag_ref[...]
    cosine = cos_ref[...]
    first_lead = jnp.sqrt(2.0 * order_real + 3.0)
    halves = rows_ref.shape[0]

    def advance(degree, carry):
        previous, older = carry
        degree_real = degree.astype(jnp.float32)
        lead = jnp.sqrt(
            jnp.maximum(4.0 * degree_real * degree_real - 1.0, 0.0)
            / jnp.maximum(degree_real * degree_real - squared, 1.0)
        )
        lower = degree_real - 1.0
        back = jnp.sqrt(
            jnp.maximum(lower * lower - squared, 0.0) / jnp.maximum(4.0 * lower * lower - 1.0, 1.0)
        )
        general = lead * (cosine * previous - back * older)
        first = first_lead * cosine * previous
        value = jnp.where(
            degree_real == order_real,
            diagonal,
            jnp.where(
                degree_real == order_real + 1.0,
                first,
                jnp.where(degree_real > order_real + 1.0, general, 0.0),
            ),
        )
        slot = slot_ref[degree]
        for half in range(halves):
            rows_ref[half, pl.ds(slot, orders, stride=degrees), :] = value[
                :, half * LANES : (half + 1) * LANES
            ]
        return (value, previous)

    zeros = diagonal * 0.0
    lax.fori_loop(0, degrees, advance, (zeros, zeros), unroll=4)
    quadrature = quad_ref[...]
    for order in range(orders):
        for half in range(halves):
            low = half * LANES
            high = min(lats, low + LANES)
            chosen = rows_ref[half, order * degrees : (order + 1) * degrees, :][:, : high - low]
            p_ref[order, :, low:high] = chosen.astype(jnp.bfloat16)
            q_ref[order, :, low:high] = (chosen * quadrature[:, low:high]).astype(jnp.bfloat16)


def spectral_tables(start, ord_dev, degree_of):
    halves = -(-LATS // LANES)
    padded = halves * LANES
    order_col = (start + jnp.arange(ord_dev, dtype=jnp.int32)).astype(jnp.float32)[:, None]
    lat_ids = jnp.minimum(jnp.arange(padded, dtype=jnp.float32), LATS - 1.0)
    colatitude = jnp.pi * (lat_ids + 0.5) / LATS
    sine = jnp.sin(colatitude)[None, :]
    steps_up = jnp.arange(1, DEGREES + 1, dtype=jnp.float32)[None, :]
    factor = jnp.where(
        steps_up <= order_col, 0.5 * jnp.log((2.0 * steps_up + 1.0) / (2.0 * steps_up)), 0.0
    )
    log_start = 0.5 * jnp.log(1.0 / (4.0 * jnp.pi)) + jnp.sum(factor, axis=1, keepdims=True)
    diagonal = jnp.exp(log_start + order_col * jnp.log(sine))
    cosine = jnp.broadcast_to(jnp.cos(colatitude)[None, :], diagonal.shape)
    quadrature = 2.0 * jnp.pi * jnp.pi / LATS * sine
    orders = jnp.broadcast_to(order_col, diagonal.shape)
    vmem = pl.BlockSpec(memory_space=pltpu.VMEM)
    shape = jax.ShapeDtypeStruct((ord_dev, DEGREES, LATS), jnp.bfloat16)
    return pl.pallas_call(
        table_kernel,
        out_shape=(shape, shape),
        in_specs=[pl.BlockSpec(memory_space=pltpu.SMEM)] + [vmem] * 4,
        out_specs=(vmem, vmem),
        scratch_shapes=[
            pltpu.SMEM((DEGREES,), jnp.int32),
            pltpu.VMEM((halves, ord_dev * DEGREES, LANES), jnp.float32),
        ],
        name="legendre_tables",
    )(degree_of, diagonal, cosine, quadrature, orders)


def fourier_tables(lon_count, order_count):
    lon_ids = jnp.arange(lon_count, dtype=jnp.int32)[:, None]
    order_ids = jnp.arange(order_count, dtype=jnp.int32)[None, :]
    phase = 2.0 * jnp.pi * (lon_ids * order_ids % lon_count).astype(jnp.float32) / lon_count
    forward = (
        jnp.stack([jnp.cos(phase), -jnp.sin(phase)], axis=2).reshape(lon_count, 2 * order_count)
        / lon_count
    )
    doubled = jnp.where(order_ids == 0, 1.0, 2.0)
    inverse = jnp.stack([doubled * jnp.cos(phase), -doubled * jnp.sin(phase)], axis=2).reshape(
        lon_count, 2 * order_count
    )
    return (forward.astype(jnp.bfloat16), jnp.transpose(inverse).astype(jnp.bfloat16))


def to_orders(values):
    return lax.all_to_all(values, "lat", split_axis=1, concat_axis=0, tiled=True)


def to_degrees(values):
    return lax.all_to_all(values, "lat", split_axis=0, concat_axis=1, tiled=True)


def back_to_orders(values):
    return lax.all_to_all(values, "lat", split_axis=1, concat_axis=0, tiled=True)


def to_bands(values):
    return lax.all_to_all(values, "lat", split_axis=0, concat_axis=1, tiled=True)


def product(spec, left, right):
    return jnp.einsum(spec, left, right, preferred_element_type=jnp.float32)


def apply_filter(coeffs, weights):
    c_real = coeffs[:, :, 0]
    c_imag = coeffs[:, :, 1]
    w_real = weights[:, 0]
    w_imag = weights[:, 1]
    f_real = product("jmsc,jcd->jmsd", c_real, w_real) - product("jmsc,jcd->jmsd", c_imag, w_imag)
    f_imag = product("jmsc,jcd->jmsd", c_real, w_imag) + product("jmsc,jcd->jmsd", c_imag, w_real)
    return jnp.stack([f_real, f_imag], axis=2).astype(jnp.bfloat16)


def adjoint_filter(grads, weights):
    g_real = grads[:, :, 0]
    g_imag = grads[:, :, 1]
    w_real = weights[:, 0]
    w_imag = weights[:, 1]
    a_real = product("jmsd,jcd->jmsc", g_real, w_real) + product("jmsd,jcd->jmsc", g_imag, w_imag)
    a_imag = product("jmsd,jcd->jmsc", g_imag, w_real) - product("jmsd,jcd->jmsc", g_real, w_imag)
    return jnp.stack([a_real, a_imag], axis=2).astype(jnp.bfloat16)


def filter_grad(coeffs, grads):
    c_real = coeffs[:, :, 0]
    c_imag = coeffs[:, :, 1]
    g_real = grads[:, :, 0]
    g_imag = grads[:, :, 1]
    dw_real = product("jmsc,jmsd->jcd", c_real, g_real) + product("jmsc,jmsd->jcd", c_imag, g_imag)
    dw_imag = product("jmsc,jmsd->jcd", c_real, g_imag) - product("jmsc,jmsd->jcd", c_imag, g_real)
    return jnp.stack([dw_real, dw_imag], axis=1)


def constant_tables(orders):
    padded = -(-LATS // LANES) * LANES
    lat_ids = np.minimum(np.arange(padded), LATS - 1)
    colatitude = np.pi * (lat_ids + 0.5) / LATS
    sine = np.sin(colatitude)[None, :]
    ids = np.arange(ORDERS)
    steps_up = np.arange(1, ORDERS + 1)
    growth = np.cumsum(0.5 * np.log((2.0 * steps_up + 1.0) / (2.0 * steps_up)))
    log_start = 0.5 * np.log(1.0 / (4.0 * np.pi)) + np.concatenate([[0.0], growth[:-1]])
    diagonal = np.exp(log_start[:, None] + ids[:, None] * np.log(sine))
    cosine = np.broadcast_to(np.cos(colatitude)[None, :], (orders, padded))
    quadrature = 2.0 * np.pi * np.pi / LATS * sine
    phase = 2.0 * np.pi * (np.arange(LONS)[:, None] * ids[None, :] % LONS) / LONS
    forward = np.stack([np.cos(phase), -np.sin(phase)], axis=2).reshape(LONS, -1) / LONS
    doubled = np.where(ids == 0, 1.0, 2.0)[None, :]
    inverse = np.stack([doubled * np.cos(phase), -doubled * np.sin(phase)], axis=2)
    inverse = inverse.reshape(LONS, -1)
    floats = [jnp.asarray(t, jnp.float32) for t in (diagonal, cosine, quadrature)]
    waves = [forward.T, forward, inverse.T, inverse]
    halves = [jnp.asarray(np.float32(t).astype(jnp.bfloat16)) for t in waves]
    return floats, halves


def fill_tables(first_order, deg_ref, diag_ref, cos_ref, quad_ref, qtab, ptab, table, by_slot):
    orders, degrees, lats = qtab.shape
    halves = by_slot.shape[0]
    diagonal = diag_ref[pl.ds(pl.multiple_of(first_order, orders), orders), :]
    cosine = cos_ref[...]
    order_ids = first_order + lax.broadcasted_iota(jnp.int32, diagonal.shape, 0)
    order_real = order_ids.astype(jnp.float32)
    squared = order_real * order_real
    first_lead = jnp.sqrt(2.0 * order_real + 3.0)

    def advance(degree, carry):
        previous, older = carry
        degree_real = degree.astype(jnp.float32)
        lead = jnp.sqrt(
            jnp.maximum(4.0 * degree_real * degree_real - 1.0, 0.0)
            / jnp.maximum(degree_real * degree_real - squared, 1.0)
        )
        lower = degree_real - 1.0
        back = jnp.sqrt(
            jnp.maximum(lower * lower - squared, 0.0) / jnp.maximum(4.0 * lower * lower - 1.0, 1.0)
        )
        general = lead * (cosine * previous - back * older)
        first = first_lead * cosine * previous
        value = jnp.where(
            order_ids == degree,
            diagonal,
            jnp.where(
                order_ids + 1 == degree, first, jnp.where(order_ids + 1 < degree, general, 0.0)
            ),
        )
        table[degree] = value
        return (value, previous)

    zeros = diagonal * 0.0
    lax.fori_loop(0, degrees, advance, (zeros, zeros), unroll=2)

    def place(slot, carry):
        value = table[deg_ref[slot]]
        for half in range(halves):
            by_slot[half, pl.ds(slot, orders, stride=degrees), :] = value[
                :, half * LANES : (half + 1) * LANES
            ]
        return carry

    lax.fori_loop(0, degrees, place, 0)
    quadrature = quad_ref[...]
    for order in range(orders):
        for half in range(halves):
            low = half * LANES
            high = min(lats, low + LANES)
            chosen = by_slot[half, order * degrees : (order + 1) * degrees, :][:, : high - low]
            ptab[order, :, low:high] = chosen.astype(jnp.bfloat16)
            qtab[order, :, low:high] = (chosen * quadrature[:, low:high]).astype(jnp.bfloat16)


def pair_swap(values, even_sign):
    rows = values.shape[0]
    even = lax.broadcasted_iota(jnp.int32, values.shape, 0) % 2 == 0
    above = pltpu.roll(values, rows - 1, 0)
    below = pltpu.roll(values, 1, 0)
    return jnp.where(even, even_sign * above, -even_sign * below)


def gelu_slope(x):
    scale = 0.7978845608028654
    square = x * x
    t = jnp.tanh(scale * (x + 0.044715 * x * square))
    return 0.5 * (1.0 + t) + 0.5 * x * (1.0 - t * t) * (scale * (1.0 + 0.134145 * square))


def dot(left, right, dims=((1,), (0,))):
    return lax.dot_general(left, right, (dims, ((), ())), preferred_element_type=jnp.float32)


def block_kernel(
    n, nb, fields, cotangent, weights, deg_ref, diag_ref, cos_ref, quad_ref,
    fwd_fk, fwd_kf, inv_fk, inv_kf,
    grad_out, dw_out,
    fbuf, cbuf, wbuf, band_out, band_in, ord_in, ord_out, deg_out, deg_back, co, go, mixed,
    wide_a, wide_b, dw, dw_in, qtab, ptab, table, by_slot,
    load_sem, send_sem, recv_sem, dw_send, dw_recv, out_sem,
):
    me = lax.axis_index("lat")
    me_b = lax.axis_index("batch")
    chunks, lat_dev = fbuf.shape[0], fbuf.shape[1]
    orders = qtab.shape[0]
    rows = 2 * orders
    slots = co.shape[1]
    degrees = n * slots
    lats = n * lat_dev
    mesh_id = pl.DeviceIdType.MESH

    def lanes(chunk):
        return pl.ds(chunk * LANES, LANES)

    def load(chunk):
        return pltpu.make_async_copy(
            fields.at[0, :, :, lanes(chunk)], fbuf.at[chunk], load_sem.at[chunk]
        )

    def load_cot(chunk):
        return pltpu.make_async_copy(
            cotangent.at[0, :, :, lanes(chunk)], cbuf.at[chunk], load_sem.at[chunks + chunk]
        )

    load_w = pltpu.make_async_copy(weights, wbuf, load_sem.at[2 * chunks])
    for chunk in range(chunks):
        load(chunk).start()
    load_w.start()
    for chunk in range(chunks):
        load_cot(chunk).start()

    barrier = pltpu.get_barrier_semaphore()

    def greet(step, carry):
        peer = lax.rem(me + step, n)
        pl.semaphore_signal(barrier, inc=1, device_id={"lat": peer}, device_id_type=mesh_id)
        return carry

    lax.fori_loop(1, n, greet, 0)
    for step in range(1, nb):
        peer = lax.rem(me_b + step, nb)
        pl.semaphore_signal(barrier, inc=1, device_id={"batch": peer}, device_id_type=mesh_id)
    pl.semaphore_wait(barrier, n - 1 + nb - 1)

    def part(ref, chunk, kind, owner):
        if kind == "band":
            return ref.at[chunk, :, pl.ds(pl.multiple_of(owner * rows, rows), rows), :]
        if kind == "lat":
            return ref.at[chunk, pl.ds(owner * lat_dev, lat_dev)]
        return ref.at[chunk, pl.ds(owner * slots, slots)]

    def exchange(stage, chunk, source, source_kind, target, target_kind):
        def send(step, carry):
            peer = lax.rem(me + 1 + lax.rem(step + n // 2 - 2, n - 1), n)
            pltpu.make_async_remote_copy(
                src_ref=part(source, chunk, source_kind, peer),
                dst_ref=part(target, chunk, target_kind, me),
                send_sem=send_sem.at[stage, chunk],
                recv_sem=recv_sem.at[stage, chunk],
                device_id={"lat": peer},
                device_id_type=mesh_id,
            ).start()
            return carry

        lax.fori_loop(1, n, send, 0)
        pltpu.make_async_copy(
            part(source, chunk, source_kind, me),
            part(target, chunk, target_kind, me),
            recv_sem.at[stage, chunk],
        ).start()

    def arrived(stage, chunk, target):
        pltpu.make_async_copy(target.at[chunk], target.at[chunk], recv_sem.at[stage, chunk]).wait()

    def departed(stage, chunk, source, kind):
        if kind == "band":
            view = source.at[chunk, :, 0 : (n - 1) * rows, :]
        elif kind == "lat":
            view = source.at[chunk, 0 : (n - 1) * lat_dev]
        else:
            view = source.at[chunk, 0 : (n - 1) * slots]
        pltpu.make_async_copy(view, view, send_sem.at[stage, chunk]).wait()

    def widen(source, chunk, depth):
        def one(block, carry):
            piece = source[chunk, pl.ds(block * depth, depth)].astype(jnp.float32)
            wide_a[pl.ds(pl.multiple_of(block * depth * rows, depth * rows), depth * rows), :] = (
                piece.reshape(depth * rows, LANES)
            )
            return carry

        lax.fori_loop(0, n, one, 0)

    def narrow(target, chunk, depth):
        def one(block, carry):
            start = pl.multiple_of(block * depth * rows, depth * rows)
            piece = wide_b[pl.ds(start, depth * rows), :]
            target[chunk, pl.ds(block * depth, depth)] = piece.reshape(
                depth, rows, LANES
            ).astype(jnp.bfloat16)
            return carry

        lax.fori_loop(0, n, one, 0)

    def apply_table(table, depth_in, depth_out, dims):
        def one(order, carry):
            real = wide_a[pl.ds(2 * order, depth_in, stride=rows), :]
            imag = wide_a[pl.ds(2 * order + 1, depth_in, stride=rows), :]
            both = jnp.concatenate([real, imag], axis=1).astype(jnp.bfloat16)
            result = dot(table[order], both, dims)
            wide_b[pl.ds(2 * order, depth_out, stride=rows), :] = result[:, :LANES]
            wide_b[pl.ds(2 * order + 1, depth_out, stride=rows), :] = result[:, LANES:]
            return carry

        lax.fori_loop(0, orders, one, 0)

    def analyse(stage, chunk, table, target, before):
        arrived(stage, chunk, ord_in)
        widen(ord_in, chunk, lat_dev)
        apply_table(table, lats, degrees, ((1,), (0,)))
        if before is not None:
            departed(before, chunk, deg_out, "slot")
        narrow(deg_out, chunk, slots)
        exchange(stage + 1, chunk, deg_out, "slot", target, "band")

    def synthesise(stage, chunk, table, before):
        arrived(stage, chunk, deg_back)
        widen(deg_back, chunk, slots)
        apply_table(table, degrees, lats, ((0,), (0,)))
        if before is not None:
            departed(before, chunk, ord_out, "lat")
        narrow(ord_out, chunk, lat_dev)
        exchange(stage + 1, chunk, ord_out, "lat", band_in, "band")

    def pair(source, chunk, row):
        return jnp.concatenate([source[chunk, 2 * row], source[chunk, 2 * row + 1]], axis=1)

    def put_pair(target, chunk, row, values):
        values = values.astype(jnp.bfloat16)
        target[chunk, 2 * row] = values[:, :LANES]
        target[chunk, 2 * row + 1] = values[:, LANES:]

    def joined(source, slot):
        return jnp.concatenate([source[chunk, slot] for chunk in range(chunks)], axis=1)

    for chunk in range(chunks):
        load(chunk).wait()

        def fourier(row, carry):
            put_pair(band_out, chunk, row, dot(fwd_fk[...], pair(fbuf, chunk, row)))
            return carry

        lax.fori_loop(0, lat_dev // 2, fourier, 0)
        exchange(0, chunk, band_out, "band", ord_in, "lat")
    fill_tables(
        me * orders, deg_ref, diag_ref, cos_ref, quad_ref, qtab, ptab, table, by_slot
    )
    for chunk in range(chunks):
        analyse(0, chunk, qtab, co, None)
    load_w.wait()
    for chunk in range(chunks):
        arrived(1, chunk, co)
    for chunk in range(chunks):

        def mix(slot, carry):
            values = joined(co, slot)
            span = slice(chunk * LANES, (chunk + 1) * LANES)
            both = dot(
                values, jnp.concatenate([wbuf[slot, 0, :, span], wbuf[slot, 1, :, span]], axis=1)
            )
            crossed = pair_swap(both[:, LANES:], -1.0)
            mixed[chunk, slot] = (both[:, :LANES] + crossed).astype(jnp.bfloat16)
            return carry

        lax.fori_loop(0, slots, mix, 0)
        exchange(2, chunk, mixed, "band", deg_back, "slot")
    for chunk in range(chunks):
        synthesise(2, chunk, ptab, None)
    for chunk in range(chunks):
        load_cot(chunk).wait()
        arrived(3, chunk, band_in)
        departed(0, chunk, band_out, "band")

        def middle(row, carry):
            response = dot(inv_kf[...], pair(band_in, chunk, row))
            upstream = pair(cbuf, chunk, row).astype(jnp.float32) * gelu_slope(response)
            put_pair(band_out, chunk, row, dot(inv_fk[...], upstream.astype(jnp.bfloat16)))
            return carry

        lax.fori_loop(0, lat_dev // 2, middle, 0)
        exchange(4, chunk, band_out, "band", ord_in, "lat")
    for chunk in range(chunks):
        analyse(4, chunk, ptab, go, 1)
    for chunk in range(chunks):
        arrived(5, chunk, go)
    for chunk in range(chunks):
        departed(2, chunk, mixed, "band")

        def adjoint(slot, carry):
            values = joined(go, slot)
            span = slice(chunk * LANES, (chunk + 1) * LANES)
            both = dot(
                values,
                jnp.concatenate([wbuf[slot, 0, span, :], wbuf[slot, 1, span, :]], axis=0),
                ((1,), (1,)),
            )
            crossed = pair_swap(both[:, LANES:], 1.0)
            mixed[chunk, slot] = (both[:, :LANES] + crossed).astype(jnp.bfloat16)
            return carry

        lax.fori_loop(0, slots, adjoint, 0)
        exchange(6, chunk, mixed, "band", deg_back, "slot")

    def weight_grad(slot, carry):
        values = joined(co, slot)
        grads = joined(go, slot)
        turned = pair_swap(grads.astype(jnp.float32), 1.0).astype(jnp.bfloat16)
        span = ((0,), (0,))
        dw[slot, 0] = dot(values, grads, span).astype(jnp.bfloat16)
        dw[slot, 1] = dot(values, turned, span).astype(jnp.bfloat16)
        return carry

    lax.fori_loop(0, slots, weight_grad, 0)
    dw_copies = []
    for step in range(1, nb):
        peer = lax.rem(me_b + step, nb)
        copy = pltpu.make_async_remote_copy(
            src_ref=dw,
            dst_ref=dw_in.at[step - 1],
            send_sem=dw_send.at[step - 1],
            recv_sem=dw_recv.at[step - 1],
            device_id={"batch": peer},
            device_id_type=mesh_id,
        )
        copy.start()
        dw_copies.append(copy)
    for chunk in range(chunks):
        synthesise(6, chunk, qtab, 3)
    for copy in dw_copies:
        copy.wait()

    def total(slot, carry):
        value = dw[slot].astype(jnp.float32)
        for step in range(nb - 1):
            value = value + dw_in[step, slot].astype(jnp.float32)
        dw[slot] = value.astype(jnp.bfloat16)
        return carry

    lax.fori_loop(0, slots, total, 0)
    store_w = pltpu.make_async_copy(dw, dw_out, out_sem.at[chunks])
    store_w.start()

    def store(chunk):
        return pltpu.make_async_copy(
            cbuf.at[chunk], grad_out.at[0, :, :, lanes(chunk)], out_sem.at[chunk]
        )

    for chunk in range(chunks):
        arrived(7, chunk, band_in)

        def finish(row, carry):
            delta = dot(fwd_kf[...], pair(band_in, chunk, row))
            put_pair(cbuf, chunk, row, pair(cbuf, chunk, row).astype(jnp.float32) + delta)
            return carry

        lax.fori_loop(0, lat_dev // 2, finish, 0)
        store(chunk).start()
    for chunk in range(chunks):
        departed(4, chunk, band_out, "band")
        departed(5, chunk, deg_out, "slot")
        departed(6, chunk, mixed, "band")
        departed(7, chunk, ord_out, "lat")
        store(chunk).wait()
    store_w.wait()


def local_kernel(fields, cotangent, weights, degree_of):
    if fields.shape[0] != 1 or fields.shape[1] % 2:
        return local(fields, cotangent, weights, degree_of)
    n = lax.axis_size("lat")
    nb = lax.axis_size("batch")
    lat_dev, lons, channels = fields.shape[1:]
    slots = weights.shape[0]
    orders = ORDERS // n
    rows = 2 * orders
    chunks = channels // LANES
    floats, waves = constant_tables(orders)
    halves = -(-LATS // LANES)
    vmem = pl.BlockSpec(memory_space=pltpu.VMEM)
    anywhere = pl.BlockSpec(memory_space=pl.ANY)

    def buffer(*dims):
        return pltpu.VMEM(dims, jnp.bfloat16)

    dma = pltpu.SemaphoreType.DMA
    others = max(nb - 1, 1)
    wide_rows = max(LATS, DEGREES) * rows
    return pl.pallas_call(
        functools.partial(block_kernel, n, nb),
        out_shape=(
            jax.ShapeDtypeStruct(fields.shape, jnp.bfloat16),
            jax.ShapeDtypeStruct(weights.shape, jnp.bfloat16),
        ),
        in_specs=[anywhere] * 3 + [pl.BlockSpec(memory_space=pltpu.SMEM)] + [vmem] * 7,
        out_specs=(anywhere, anywhere),
        scratch_shapes=[
            buffer(chunks, lat_dev, lons, LANES),
            buffer(chunks, lat_dev, lons, LANES),
            buffer(*weights.shape),
            buffer(chunks, lat_dev, n * rows, LANES),
            buffer(chunks, lat_dev, n * rows, LANES),
            buffer(chunks, LATS, rows, LANES),
            buffer(chunks, LATS, rows, LANES),
            buffer(chunks, DEGREES, rows, LANES),
            buffer(chunks, DEGREES, rows, LANES),
            buffer(chunks, slots, n * rows, LANES),
            buffer(chunks, slots, n * rows, LANES),
            buffer(chunks, slots, n * rows, LANES),
            pltpu.VMEM((wide_rows, LANES), jnp.float32),
            pltpu.VMEM((wide_rows, LANES), jnp.float32),
            buffer(*weights.shape),
            buffer(others, *weights.shape),
            buffer(orders, DEGREES, LATS),
            buffer(orders, DEGREES, LATS),
            pltpu.VMEM((DEGREES, orders, halves * LANES), jnp.float32),
            pltpu.VMEM((halves, orders * DEGREES, LANES), jnp.float32),
            dma((2 * chunks + 1,)),
            dma((8, chunks)),
            dma((8, chunks)),
            dma((others,)),
            dma((others,)),
            dma((chunks + 1,)),
        ],
        compiler_params=pltpu.CompilerParams(
            collective_id=0, has_side_effects=True, vmem_limit_bytes=60 * 2**20
        ),
        name="filter_block",
    )(
        fields, cotangent, weights, degree_of, *floats, *waves,
    )


def local(fields, cotangent, weights, degree_of):
    samples = fields.shape[0]
    band_rows = fields.shape[1]
    ord_dev = ORDERS // lax.axis_size("lat")
    forward, inverse = fourier_tables(LONS, ORDERS)
    qslot, pslot = spectral_tables(lax.axis_index("lat") * ord_dev, ord_dev, degree_of)
    spectra = product("sikc,kf->ifsc", fields, forward).astype(jnp.bfloat16)
    spectra = spectra.reshape(band_rows, ORDERS, 2, samples, CHANNELS)
    gathered = to_orders(spectra)
    coeffs_local = product("mji,imrsc->jmrsc", qslot, gathered).astype(jnp.bfloat16)
    coeffs = to_degrees(coeffs_local)
    filtered = apply_filter(coeffs, weights)
    returned = back_to_orders(filtered)
    synth_local = product("mji,jmrsc->imrsc", pslot, returned).astype(jnp.bfloat16)
    synth = to_bands(synth_local)
    response = product(
        "ifsc,fk->sikc", synth.reshape(band_rows, 2 * ORDERS, samples, CHANNELS), inverse
    )
    activated, pullback = jax.vjp(jax.nn.gelu, response)
    upstream = pullback(cotangent.astype(jnp.float32))[0].astype(jnp.bfloat16)
    grad_synth = product("sikc,fk->ifsc", upstream, inverse).astype(jnp.bfloat16)
    grad_synth = grad_synth.reshape(band_rows, ORDERS, 2, samples, CHANNELS)
    grad_gathered = to_orders(grad_synth)
    grad_local = product("mji,imrsc->jmrsc", pslot, grad_gathered).astype(jnp.bfloat16)
    grad_filtered = to_degrees(grad_local)
    weight_total = lax.psum(filter_grad(coeffs, grad_filtered).astype(jnp.bfloat16), "batch")
    grad_coeffs = adjoint_filter(grad_filtered, weights)
    grad_back = back_to_orders(grad_coeffs)
    grad_local_spec = product("mji,jmrsc->imrsc", qslot, grad_back).astype(jnp.bfloat16)
    grad_bands = to_bands(grad_local_spec)
    delta = product(
        "ifsc,kf->sikc", grad_bands.reshape(band_rows, 2 * ORDERS, samples, CHANNELS), forward
    )
    grad_fields = (cotangent.astype(jnp.float32) + delta).astype(jnp.bfloat16)
    return (grad_fields, weight_total)


def solution(mesh):
    orders = ORDERS // mesh.shape["lat"]
    return jax.shard_map(
        local_kernel if orders % 8 == 0 and CHANNELS % LANES == 0 else local,
        mesh=mesh,
        in_specs=(
            P("batch", "lat", None, None),
            P("batch", "lat", None, None),
            P("lat", None, None, None),
            P(),
        ),
        out_specs=(P("batch", "lat", None, None), P("lat", None, None, None)),
        check_vma=False,
    )
```
